32 devices in a mesh: groups: 2 (over x), seq: 16 (over z, y, core).
Axes of the slice: x: 2, y: 2, z: 4, core: 2. Of those that a mesh axis runs over, the one named last changes fastest.
Arguments:
- query: bfloat16 [16, 4096], P('groups'), parts along dimension 0, may hold values from -12 to 12
- new_key: bfloat16 [16, 1024], P('groups'), parts along dimension 0, may hold values from -12 to 12
- new_value: bfloat16 [16, 1024], P('groups'), parts along dimension 0, may hold values from -12 to 12
- cache_keys: bfloat16 [16, 1024, 1024], P('groups', 'seq'), parts along dimension 0, may hold values from -6 to 6
- cache_values: bfloat16 [16, 1024, 1024], P('groups', 'seq'), parts along dimension 0, may hold values from -6 to 6
- cache_lengths: int32 [16], P('groups'), parts along dimension 0, may hold values from 512 to 1024
- residual_input: bfloat16 [16, 4096], P('groups'), parts along dimension 0, may hold values from -6 to 6
- w_out: bfloat16 [4096, 4096], P('seq'), may hold values from -0.09375 to 0.09375
- norm_gain: bfloat16 [4096], replicated, may hold values from 0.099609375 to 1.8984375
- w_router: bfloat16 [4096, 4], replicated, may hold values from -0.09375 to 0.09375
- w_gate: bfloat16 [4096, 28672], P(None, 'seq'), may hold values from -0.09375 to 0.09375
- w_up: bfloat16 [4096, 28672], P(None, 'seq'), may hold values from -0.09375 to 0.09375
- expert_down_weight: bfloat16 [28672, 4096], P('seq'), may hold values from -0.09375 to 0.09375
- expert_ids: int32 [16, 2], P('groups'), parts along dimension 0, may hold values from 0 to 3, all different within a row
Outputs:
- attn_proj: bfloat16 [16, 4096], P('groups', 'seq'), parts along dimension 0
- layer_out: bfloat16 [16, 4096], P('groups', 'seq'), parts along dimension 0
The draws below stay inside these ranges and needn't reach their ends.
There are 2 independent parts, one for each index of `groups`. The reference program is written for one: setup_inputs(seed, part) draws one part's arguments, and reference() takes and returns one part's arrays. A program takes and returns all parts, laid end to end along the dimension named above; an argument that names none is the same for every part. Nothing has to cross between parts.
Inputs may be any that keep to these rules, and one draw needn't show every extreme that they name: Cache positions 0 to cache_lengths[b] - 1 of sequence b are live, the rest are not read; the new key and value are always live. `expert_ids`: the two experts of a token differ.
All inputs are finite; a program needn't handle non-finite values.
Results may differ from the reference program's by a relative error of at most 0.012.
Values sent between devices are 32-bit elements; how exact they have to be, the bound alone decides.
A program may use at most 128 MiB of HBM per device.

```python
import math
import jax
import jax.numpy as jnp
from jax import lax

D = 4096
HEADS = 32
KV_HEADS = 8
HEAD_DIM = 128
EXPERTS = 4
FF = 7168
SEQS = 8
CACHE = 1024


def draw_query(key, part):
    shape = (SEQS, HEADS * HEAD_DIM)
    values_base = 2.0 * jax.random.truncated_normal(jax.random.fold_in(key, 1), -6.0, 6.0, shape, jnp.float32)
    return values_base.astype(jnp.bfloat16)


def draw_cache_keys(key, part):
    shape = (SEQS, CACHE, KV_HEADS * HEAD_DIM)
    values_base = jax.random.truncated_normal(jax.random.fold_in(key, 2), -6.0, 6.0, shape, jnp.float32)
    return values_base.astype(jnp.bfloat16)


def touch_ends(drawn, rng, low, largest):
    extent = drawn.shape
    index_at = [jax.random.randint(jax.random.fold_in(rng, axis), (), 0, extent[axis]) for axis in range(len(extent))]
    drawn = drawn.at[tuple(index_at)].set(low)
    longest = extent.index(max(extent))
    index_at[longest] = (index_at[longest] + 1) % extent[longest]
    return drawn.at[tuple(index_at)].set(largest)


def strengthened(values, key, source, target, blocks, factor):
    owner, partner = [(jnp.arange(values.shape[axis_at]) // (values.shape[axis_at] // blocks)).reshape([-1 if axis == axis_at else 1 for axis in range(values.ndim)]) for axis_at in (source, target)]
    chosen = jax.random.permutation(key, blocks)[partner]
    strong = (owner == chosen) | (owner == (partner + blocks // 2) % blocks)
    return jnp.where(strong, factor * values, values)


def shard_levels(key, shape, shards, low, largest):
    def one(dim, parts):
        steps = jax.random.uniform(jax.random.fold_in(jax.random.fold_in(key, 6), dim), (parts,), jnp.float32, low / len(shards), largest / len(shards))
        return jnp.repeat(jnp.exp(steps), shape[dim] // parts).reshape((-1,) + (1,) * (len(shape) - dim - 1))

    gain = one(*shards[0])
    for cut in shards[1:]:
        gain = gain * one(*cut)
    return gain


def distinct(rng, rows, count, top, lift):
    order = jax.random.permutation(jax.random.fold_in(rng, 1), count)
    pull = order
    for power in range(3):
        pull = pull * pull // count
    pull = pull * lift // count
    tickets = jax.random.randint(jax.random.fold_in(rng, 2), (rows, count), 0, 4096) + pull
    sure = jax.random.permutation(jax.random.fold_in(rng, 3), rows)[jnp.arange(count) % rows]
    tickets = jnp.where(jnp.arange(rows)[:, None] == sure[None, :], 1 << 14, tickets)
    score = tickets * count + jnp.arange(count)
    return lax.top_k(score.astype(jnp.int32), top)[1].astype(jnp.int32)


def gaussian(key, extent, spread, bound, split=(), kind=jnp.bfloat16):
    drawn = jax.random.normal(key, extent, jnp.float32) * spread
    if len(split) > 0:
        drawn = shard_levels(key, extent, split, -0.22, 0.18) * drawn
    return jnp.clip(drawn, min=-bound, max=bound).astype(kind)


def heavy_noise(rng, extent, spread, bound, pieces, heavy, held_as=jnp.bfloat16):
    entries = spread * jax.random.normal(rng, extent, jnp.float32)
    if pieces:
        entries = entries * shard_levels(rng, extent, pieces, -0.22, 0.18)
    return jnp.clip(strengthened(entries, jax.random.fold_in(rng, 3), *heavy), -bound, bound).astype(held_as)


def setup_inputs(seed: int = 0, part: int = 0) -> dict:
    key_of = jax.random.split(jax.random.key(seed), 15)
    part_keys = jax.random.split(jax.random.fold_in(key_of[14], part), 15)
    query = draw_query(jax.random.fold_in(jax.random.fold_in(key_of[14], part), 71), part)
    new_key = gaussian(part_keys[1], (SEQS, KV_HEADS * HEAD_DIM), 2.0, 12.0)
    new_value = gaussian(part_keys[2], (SEQS, KV_HEADS * HEAD_DIM), 2.0, 12.0)
    cache_keys = draw_cache_keys(jax.random.fold_in(jax.random.fold_in(key_of[14], part), 71), part)
    cache_values = gaussian(part_keys[4], (SEQS, CACHE, KV_HEADS * HEAD_DIM), 1.0, 6.0, ((1, 16),))
    cache_lengths = touch_ends(jax.random.randint(part_keys[5], (SEQS,), CACHE // 2, CACHE + 1), jax.random.fold_in(part_keys[5], 1), CACHE // 2, CACHE).astype(jnp.int32)
    residual_input = gaussian(part_keys[6], (SEQS, D), 1.0, 6.0)
    w_out = gaussian(key_of[7], (HEADS * HEAD_DIM, D), (HEADS * HEAD_DIM) ** -0.5, 0.09375, ((0, 16),))
    norm_gain = jnp.clip(1.0 + 0.18 * jax.random.normal(key_of[8], (D,), jnp.float32), 0.099609375, 1.8984375).astype(jnp.bfloat16)
    w_router = gaussian(key_of[9], (D, EXPERTS), D ** -0.5, 0.09375)
    w_gate = gaussian(key_of[10], (D, EXPERTS * FF), D ** -0.5, 0.09375, ((1, 16),))
    w_up = gaussian(key_of[11], (D, EXPERTS * FF), D ** -0.5, 0.09375, ((1, 16),))
    expert_down_weight = heavy_noise(key_of[12], (EXPERTS * FF, D), FF ** -0.5, 0.09375, ((0, 16),), (0, 1, 16, 2.0))
    expert_ids = distinct(part_keys[13], SEQS, EXPERTS, 2, 4096)
    return {"query": query, "new_key": new_key, "new_value": new_value, "cache_keys": cache_keys, "cache_values": cache_values, "cache_lengths": cache_lengths, "residual_input": residual_input, "w_out": w_out, "norm_gain": norm_gain, "w_router": w_router, "w_gate": w_gate, "w_up": w_up, "expert_down_weight": expert_down_weight, "expert_ids": expert_ids}


masked_score = -1e+30

def attend_sequence(packed):
    query_row, cached_key_matrix, value_rows, length, fresh_key, fresh_value = packed
    per_group = HEADS // KV_HEADS
    inv_scale = 1.0 / math.sqrt(HEAD_DIM)
    query_vectors = query_row.astype(jnp.float32).reshape(KV_HEADS, per_group, HEAD_DIM)
    key_block = cached_key_matrix.astype(jnp.float32).reshape(-1, KV_HEADS, HEAD_DIM)
    value_block = value_rows.astype(jnp.float32).reshape(-1, KV_HEADS, HEAD_DIM)
    scores = jnp.einsum('kgd,tkd->kgt', query_vectors, key_block) * inv_scale
    is_live = jnp.arange(key_block.shape[0], dtype=jnp.int32) < length
    scores = jnp.where(is_live, scores, masked_score)
    incoming_token_score = jnp.einsum('kgd,kd->kg', query_vectors, fresh_key.astype(jnp.float32).reshape(KV_HEADS, HEAD_DIM)) * inv_scale
    ceiling = jnp.maximum(lax.optimization_barrier(jnp.max(scores, axis=-1)), incoming_token_score)
    weights = jnp.where(is_live, jnp.exp(scores - ceiling[..., None]), 0.0)
    fresh_weight = jnp.exp(incoming_token_score - ceiling)
    denominator = lax.optimization_barrier(jnp.sum(weights, axis=-1)) + fresh_weight
    rounded = lax.optimization_barrier(weights.astype(jnp.bfloat16)).astype(jnp.float32)
    fresh_rounded = lax.optimization_barrier(fresh_weight.astype(jnp.bfloat16)).astype(jnp.float32)
    numerator = jnp.einsum('kgt,tkd->kgd', rounded, value_block)
    numerator = numerator + fresh_rounded[..., None] * fresh_value.astype(jnp.float32).reshape(KV_HEADS, 1, HEAD_DIM)
    return (numerator / denominator[..., None]).reshape(-1)

def reference(query, new_key, new_value, cache_keys, cache_values, cache_lengths, residual_input, w_out, norm_gain, w_router, w_gate, w_up, expert_down_weight, expert_ids):
    context = lax.map(attend_sequence, (query, cache_keys, cache_values, cache_lengths.astype(jnp.int32), new_key, new_value))
    context = context.astype(jnp.bfloat16)
    projected = jnp.dot(context, w_out, preferred_element_type=jnp.float32)
    attn_proj = projected.astype(jnp.bfloat16)
    stream = residual_input.astype(jnp.float32) + projected
    normed = stream * lax.rsqrt(lax.optimization_barrier(jnp.mean(stream * stream, axis=-1, keepdims=True)) + 1e-05) * norm_gain.astype(jnp.float32)
    normed = normed.astype(jnp.bfloat16)
    logits = jnp.dot(normed, w_router, preferred_element_type=jnp.float32)
    chosen = jnp.take_along_axis(logits, expert_ids.astype(jnp.int32), axis=1)
    first_gate = jax.nn.sigmoid(chosen[:, 0] - chosen[:, 1])
    gate_pair = jnp.stack([first_gate, 1.0 - first_gate], axis=1)
    mixture = jnp.zeros(stream.shape, jnp.float32)
    for expert in range(EXPERTS):
        gate_part = jnp.dot(normed, w_gate[:, expert * FF:(expert + 1) * FF], preferred_element_type=jnp.float32)
        up_projection_share = jnp.dot(normed, w_up[:, expert * FF:(expert + 1) * FF], preferred_element_type=jnp.float32)
        hidden = (jax.nn.silu(gate_part) * up_projection_share).astype(jnp.bfloat16)
        expert_out = jnp.dot(hidden, expert_down_weight[expert * FF:(expert + 1) * FF, :], preferred_element_type=jnp.float32)
        route_weight = lax.optimization_barrier(jnp.sum(jnp.where(expert_ids == expert, gate_pair, 0.0), axis=1))
        mixture = mixture + route_weight[:, None] * expert_out
    layer_out = (stream + mixture).astype(jnp.bfloat16)
    return (attn_proj, layer_out)
```

```python
import functools
import math

import jax
import jax.numpy as jnp
from jax import lax
from jax.experimental import pallas as pl
from jax.experimental.pallas import tpu as pltpu
from jax.sharding import PartitionSpec as P

HEADS = 32
KV_HEADS = 8
HEAD_DIM = 128
FF = 7168


masked_score = -1e30


def joined(value, axis, join):
    pieces = jax.tree.map(lambda part: lax.all_gather(part, axis), value)
    head = jax.tree.map(lambda part: part[0], pieces)
    tail = jax.tree.map(lambda part: part[1:], pieces)
    so_far, _ = lax.scan(lambda so_far, share: (join(so_far, share), None), head, tail)
    return so_far


def merge_partial_results(first, second):
    first_max, first_sum, first_num = first
    second_max, second_sum, second_num = second
    ceiling = jnp.maximum(first_max, second_max)
    first_scale = jnp.exp(first_max - ceiling)
    second_scale = jnp.exp(second_max - ceiling)
    merged_sum = first_sum * first_scale + second_sum * second_scale
    merged_num = first_num * first_scale[..., None] + second_num * second_scale[..., None]
    return (ceiling, merged_sum, merged_num)


def per_device(
    query,
    new_key,
    new_value,
    cache_keys,
    cache_values,
    cache_lengths,
    residual_input,
    w_out,
    norm_gain,
    w_router,
    w_gate,
    w_up,
    expert_down_weight,
    expert_ids,
):
    seq_count = query.shape[0]
    per_group = HEADS // KV_HEADS
    local_len = cache_keys.shape[1]
    device = lax.axis_index("seq")
    inv_scale = 1.0 / math.sqrt(HEAD_DIM)
    query_vectors = query.reshape(seq_count, KV_HEADS, per_group, HEAD_DIM)
    key_block = cache_keys.reshape(seq_count, local_len, KV_HEADS, HEAD_DIM)
    value_block = cache_values.reshape(seq_count, local_len, KV_HEADS, HEAD_DIM)
    scores = (
        jnp.einsum("bkgd,btkd->bkgt", query_vectors, key_block, preferred_element_type=jnp.float32)
        * inv_scale
    )
    positions = device * local_len + jnp.arange(local_len, dtype=jnp.int32)
    is_live = (positions[None, :] < cache_lengths[:, None])[:, None, None, :]
    scores = jnp.where(is_live, scores, masked_score)
    incoming_key_rows = new_key.reshape(seq_count, KV_HEADS, HEAD_DIM)
    incoming_token_score = (
        jnp.einsum(
            "oqes,oqs->oqe", query_vectors, incoming_key_rows, preferred_element_type=jnp.float32
        )
        * inv_scale
    )
    fresh_value = new_value.astype(jnp.float32).reshape(seq_count, KV_HEADS, 1, HEAD_DIM)
    feat_width = w_out.shape[0]
    feat_start = device * feat_width
    flat_shape = (seq_count, HEADS * HEAD_DIM)
    local_max = jnp.max(scores, axis=-1)
    weights = jnp.where(is_live, jnp.exp(scores - local_max[..., None]), 0.0)
    numerator = jnp.einsum(
        "bkgt,btkd->bkgd",
        weights.astype(jnp.bfloat16),
        value_block,
        preferred_element_type=jnp.float32,
    )
    merged_max, merged_sum, merged_num = joined(
        (local_max, jnp.sum(weights, axis=-1), numerator), "seq", merge_partial_results
    )
    ceiling = jnp.maximum(merged_max, incoming_token_score)
    old_scale = jnp.exp(merged_max - ceiling)
    fresh_weight = jnp.exp(incoming_token_score - ceiling)
    fresh_rounded = lax.optimization_barrier(fresh_weight.astype(jnp.bfloat16)).astype(jnp.float32)
    numerator = merged_num * old_scale[..., None] + fresh_rounded[..., None] * fresh_value
    denominator = merged_sum * old_scale + fresh_weight
    context = (numerator / denominator[..., None]).reshape(flat_shape)
    context_own = lax.dynamic_slice_in_dim(context, feat_start, feat_width, 1).astype(jnp.bfloat16)
    projected = lax.psum(jnp.dot(context_own, w_out, preferred_element_type=jnp.float32), "seq")
    out_width = projected.shape[1] // lax.axis_size("seq")
    out_start = device * out_width
    attn_proj = lax.dynamic_slice_in_dim(projected, out_start, out_width, 1).astype(jnp.bfloat16)
    stream = residual_input.astype(jnp.float32) + projected
    normed = (
        stream
        * lax.rsqrt(jnp.mean(stream * stream, axis=-1, keepdims=True) + 1e-05)
        * norm_gain.astype(jnp.float32)
    )
    normed = normed.astype(jnp.bfloat16)
    logits = jnp.dot(normed, w_router, preferred_element_type=jnp.float32)
    expert_count = w_router.shape[1]
    picks = expert_ids[:, :, None] == jnp.arange(expert_count, dtype=jnp.int32)[None, None, :]
    chosen = jnp.sum(jnp.where(picks, logits[:, None, :], 0.0), axis=-1)
    first_gate = jax.nn.sigmoid(chosen[:, 0] - chosen[:, 1])
    gate_pair = jnp.stack([first_gate, 1.0 - first_gate], axis=1)
    own_expert = device * w_gate.shape[1] // FF
    route_weight = jnp.sum(jnp.where(expert_ids == own_expert, gate_pair, 0.0), axis=1)
    gate_part = jnp.dot(normed, w_gate, preferred_element_type=jnp.float32)
    up_projection_share = jnp.dot(normed, w_up, preferred_element_type=jnp.float32)
    hidden = (jax.nn.silu(gate_part) * up_projection_share).astype(jnp.bfloat16)
    term = lax.dot_general(
        expert_down_weight, hidden, (((0,), (1,)), ((), ())), preferred_element_type=jnp.float32
    )
    moe_rows = lax.psum_scatter(
        term * route_weight[None, :], "seq", scatter_dimension=0, tiled=True
    )
    stream_own = lax.dynamic_slice_in_dim(stream, out_start, out_width, 1)
    layer_out = (stream_own + moe_rows.T).astype(jnp.bfloat16)
    return (attn_proj, layer_out)


def layer_kernel(
    n,
    lengths_ref,
    ids_ref,
    query_hbm,
    new_key_hbm,
    new_value_hbm,
    keys_hbm,
    values_hbm,
    residual_hbm,
    w_out_hbm,
    gain_hbm,
    router_hbm,
    gate_hbm,
    up_hbm,
    down_hbm,
    attn_out,
    layer_out,
    query,
    new_key,
    new_value,
    keys,
    values,
    residual,
    w_out,
    gain,
    router,
    w_gate,
    w_up,
    w_down,
    send_ctx,
    recv_ctx,
    send_proj,
    recv_proj,
    gathered,
    send_moe,
    recv_moe,
    normed_ref,
    hidden_ref,
    small_sem,
    gate_sem,
    up_sem,
    down_sem,
    send_sem,
    recv_sem,
):
    f32, bf16 = jnp.float32, jnp.bfloat16
    me = lax.axis_index("seq")
    seqs = query.shape[0]
    local_len = keys.shape[1]
    per_group = HEADS // KV_HEADS
    width = w_out.shape[0]
    own_heads = width // HEAD_DIM
    ff_local = w_gate.shape[1]
    inv_scale = 1.0 / math.sqrt(HEAD_DIM)

    small = [
        pltpu.make_async_copy(src, dst, small_sem.at[i])
        for i, (src, dst) in enumerate(
            (
                (query_hbm, query),
                (keys_hbm, keys),
                (values_hbm, values),
                (new_key_hbm, new_key),
                (new_value_hbm, new_value),
                (w_out_hbm, w_out),
                (residual_hbm, residual),
                (gain_hbm, gain),
                (router_hbm, router),
            )
        )
    ]
    for copy in small:
        copy.start()
    big = []
    for src, dst, sems in (
        (gate_hbm, w_gate, gate_sem),
        (up_hbm, w_up, up_sem),
        (down_hbm, w_down, down_sem),
    ):
        parts = sems.shape[0]
        rows = src.shape[0] // parts
        copies = [
            pltpu.make_async_copy(
                src.at[pl.ds(i * rows, rows)], dst.at[pl.ds(i * rows, rows)], sems.at[i]
            )
            for i in range(parts)
        ]
        for copy in copies:
            copy.start()
        big.append(copies)

    barrier = pltpu.get_barrier_semaphore()

    def greet(i, carry):
        pl.semaphore_signal(barrier, inc=1, device_id={"seq": lax.rem(me + i, n)})
        return carry

    lax.fori_loop(1, n, greet, 0)

    def exchange(phase, src, dst, peer, slot):
        return pltpu.make_async_remote_copy(
            src_ref=src,
            dst_ref=dst.at[slot],
            send_sem=send_sem.at[phase, peer],
            recv_sem=recv_sem.at[phase, slot],
            device_id={"seq": peer},
        )

    def wait_all(phase, dst):
        def step(i, carry):
            peer = lax.rem(me + i, n)
            exchange(phase, dst.at[peer], dst, peer, peer).wait_recv()
            return carry

        lax.fori_loop(1, n, step, 0)

    rows = per_group * seqs
    cols = seqs * local_len
    row_seq = lax.rem(lax.broadcasted_iota(jnp.int32, (rows, 1), 0), seqs)
    row_len = jnp.zeros((rows, 1), jnp.int32)
    for b in range(seqs):
        row_len = jnp.where(row_seq == b, lengths_ref[b], row_len)
    offset = lax.broadcasted_iota(jnp.int32, (rows, cols), 1) - row_seq * local_len
    valid = (offset >= 0) & (offset < jnp.minimum(row_len - me * local_len, local_len))
    lane = lax.broadcasted_iota(jnp.int32, (rows, HEAD_DIM), 1)

    for copy in small[:3]:
        copy.wait()
    stats = [None] * HEADS
    for k in range(KV_HEADS):
        span = slice(k * HEAD_DIM, (k + 1) * HEAD_DIM)
        grouped = jnp.concatenate(
            [
                query[:, (k * per_group + g) * HEAD_DIM : (k * per_group + g + 1) * HEAD_DIM].astype(f32)
                for g in range(per_group)
            ],
            axis=0,
        ).astype(bf16)
        key_block = keys[:, :, span].reshape(cols, HEAD_DIM)
        value_block = values[:, :, span].reshape(cols, HEAD_DIM)
        scores = (
            lax.dot_general(
                grouped, key_block, (((1,), (1,)), ((), ())), preferred_element_type=f32
            )
            * inv_scale
        )
        scores = jnp.where(valid, scores, masked_score)
        top = jnp.max(scores, axis=1, keepdims=True)
        weights = jnp.where(valid, jnp.exp(scores - top), 0.0)
        total = jnp.sum(weights, axis=1, keepdims=True)
        numerator = jnp.dot(weights.astype(bf16), value_block, preferred_element_type=f32)
        for g in range(per_group):
            head = k * per_group + g
            peer, part = head // own_heads, head % own_heads
            part_rows = slice(g * seqs, (g + 1) * seqs)
            send_ctx[peer, :, part * HEAD_DIM : (part + 1) * HEAD_DIM] = numerator[part_rows]
            stats[head] = jnp.where(
                lane[:seqs] == 2 * part,
                top[part_rows],
                jnp.where(lane[:seqs] == 2 * part + 1, total[part_rows], 0.0),
            )
    for peer in range(n):
        block = stats[peer * own_heads]
        for part in range(1, own_heads):
            block = block + stats[peer * own_heads + part]
        send_ctx[peer, :, width:] = block

    pl.semaphore_wait(barrier, n - 1)

    def send_context(i, carry):
        peer = lax.rem(me + i, n)
        exchange(0, send_ctx.at[peer], recv_ctx, peer, me).start()
        return carry

    lax.fori_loop(1, n, send_context, 0)
    recv_ctx[pl.ds(me, 1)] = send_ctx[pl.ds(me, 1)]

    for copy in small[3:5]:
        copy.wait()
    fresh = []
    for part in range(own_heads):
        head = me * own_heads + part
        kv = head // per_group
        at = pl.ds(pl.multiple_of(kv * HEAD_DIM, HEAD_DIM), HEAD_DIM)
        q_at = pl.ds(pl.multiple_of(head * HEAD_DIM, HEAD_DIM), HEAD_DIM)
        score = (
            jnp.sum(query[:, q_at].astype(f32) * new_key[:, at].astype(f32), axis=1, keepdims=True)
            * inv_scale
        )
        fresh.append((score, new_value[:, at].astype(f32)))

    wait_all(0, recv_ctx)
    pieces = []
    for part in range(own_heads):
        score, value = fresh[part]
        tops = recv_ctx[:, :, width + 2 * part : width + 2 * part + 1]
        totals = recv_ctx[:, :, width + 2 * part + 1 : width + 2 * part + 2]
        ceiling = jnp.maximum(jnp.max(tops, axis=0), score)
        scale = jnp.exp(tops - ceiling[None])
        new_weight = jnp.exp(score - ceiling)
        denominator = jnp.sum(totals * scale, axis=0) + new_weight
        numerator = jnp.sum(
            recv_ctx[:, :, part * HEAD_DIM : (part + 1) * HEAD_DIM] * scale, axis=0
        )
        numerator = numerator + new_weight.astype(bf16).astype(f32) * value
        pieces.append(numerator / denominator)
    context = jnp.concatenate(pieces, axis=1).astype(bf16)

    small[5].wait()

    def project(peer):
        at = pl.ds(pl.multiple_of(peer * width, width), width)
        return jnp.dot(context, w_out[:, at], preferred_element_type=f32)

    def send_projected(i, carry):
        peer = lax.rem(me + i, n)
        send_proj[peer] = project(peer)
        exchange(1, send_proj.at[peer], recv_proj, peer, me).start()
        return carry

    lax.fori_loop(1, n, send_projected, 0)
    recv_proj[me] = project(me)
    for copy in small[6:]:
        copy.wait()
    wait_all(1, recv_proj)
    projected = jnp.sum(recv_proj[...], axis=0)
    gathered[me] = projected

    def send_gathered(i, carry):
        peer = lax.rem(me + i, n)
        exchange(2, gathered.at[me], gathered, peer, me).start()
        return carry

    lax.fori_loop(1, n, send_gathered, 0)
    attn_out[...] = projected.astype(bf16)
    own_at = pl.ds(pl.multiple_of(me * width, width), width)
    stream_own = residual[:, own_at].astype(f32) + projected
    wait_all(2, gathered)

    stream = [
        gathered[p] + residual[:, p * width : (p + 1) * width].astype(f32) for p in range(n)
    ]
    squares = stream[0] * stream[0]
    for p in range(1, n):
        squares = squares + stream[p] * stream[p]
    inv_rms = lax.rsqrt(jnp.sum(squares, axis=1, keepdims=True) / (n * width) + 1e-05)
    for p in range(n):
        at = slice(p * width, (p + 1) * width)
        normed_ref[:, at] = (stream[p] * inv_rms * gain[:, at].astype(f32)).astype(bf16)

    normed = normed_ref[...]
    logits = lax.dot_general(
        normed, router[...], (((1,), (1,)), ((), ())), preferred_element_type=f32
    )
    expert = lax.broadcasted_iota(jnp.int32, logits.shape, 1)
    token = lax.broadcasted_iota(jnp.int32, (seqs, 1), 0)
    first_id = jnp.zeros((seqs, 1), jnp.int32)
    second_id = jnp.zeros((seqs, 1), jnp.int32)
    for b in range(seqs):
        first_id = jnp.where(token == b, ids_ref[b, 0], first_id)
        second_id = jnp.where(token == b, ids_ref[b, 1], second_id)
    first_logit = jnp.sum(jnp.where(expert == first_id, logits, 0.0), axis=1, keepdims=True)
    second_logit = jnp.sum(jnp.where(expert == second_id, logits, 0.0), axis=1, keepdims=True)
    first_gate = 1.0 / (1.0 + jnp.exp(second_logit - first_logit))
    own_expert = me * ff_local // FF
    route = jnp.where(first_id == own_expert, first_gate, 0.0) + jnp.where(
        second_id == own_expert, 1.0 - first_gate, 0.0
    )

    for copies in big[:2]:
        for copy in copies:
            copy.wait()
    tile = 256

    def hidden_step(j, carry):
        at = pl.ds(pl.multiple_of(j * tile, tile), tile)
        gate_part = jnp.dot(normed_ref[...], w_gate[:, at], preferred_element_type=f32)
        up_part = jnp.dot(normed_ref[...], w_up[:, at], preferred_element_type=f32)
        hidden_ref[:, at] = (gate_part / (1.0 + jnp.exp(-gate_part)) * up_part).astype(bf16)
        return carry

    lax.fori_loop(0, ff_local // tile, hidden_step, 0)
    for copy in big[2]:
        copy.wait()

    def contribution(peer):
        at = pl.ds(pl.multiple_of(peer * width, width), width)
        return jnp.dot(hidden_ref[...], w_down[:, at], preferred_element_type=f32) * route

    def send_contribution(i, carry):
        peer = lax.rem(me + i, n)
        send_moe[peer] = contribution(peer)
        exchange(3, send_moe.at[peer], recv_moe, peer, me).start()
        return carry

    lax.fori_loop(1, n, send_contribution, 0)
    recv_moe[me] = contribution(me)
    wait_all(3, recv_moe)
    layer_out[...] = (stream_own + jnp.sum(recv_moe[...], axis=0)).astype(bf16)

    def finish(i, carry):
        peer = lax.rem(me + i, n)
        exchange(0, send_ctx.at[peer], recv_ctx, peer, me).wait_send()
        exchange(1, send_proj.at[peer], recv_proj, peer, me).wait_send()
        exchange(2, gathered.at[me], gathered, peer, me).wait_send()
        exchange(3, send_moe.at[peer], recv_moe, peer, me).wait_send()
        return carry

    lax.fori_loop(1, n, finish, 0)


def fused_device(n, *args):
    (
        query,
        new_key,
        new_value,
        cache_keys,
        cache_values,
        cache_lengths,
        residual_input,
        w_out,
        norm_gain,
        w_router,
        w_gate,
        w_up,
        expert_down_weight,
        expert_ids,
    ) = args
    seqs, features = residual_input.shape
    width = w_out.shape[0]
    if width % HEAD_DIM or w_gate.shape[1] % 256 or width * n != features or cache_keys.shape[1] % 16:
        return per_device(*args)
    f32, bf16 = jnp.float32, jnp.bfloat16
    operands = (
        query,
        new_key,
        new_value,
        cache_keys,
        cache_values,
        residual_input,
        w_out,
        norm_gain.reshape(1, features),
        w_router.T,
        w_gate,
        w_up,
        expert_down_weight,
    )
    packet = (n, seqs, width + HEAD_DIM)
    block = (n, seqs, width)
    out = jax.ShapeDtypeStruct((seqs, width), bf16)
    return pl.pallas_call(
        functools.partial(layer_kernel, n),
        out_shape=(out, out),
        in_specs=[pl.BlockSpec(memory_space=pltpu.SMEM)] * 2
        + [pl.BlockSpec(memory_space=pl.ANY)] * len(operands),
        out_specs=(pl.BlockSpec(memory_space=pltpu.VMEM),) * 2,
        scratch_shapes=[pltpu.VMEM(x.shape, x.dtype) for x in operands]
        + [
            pltpu.VMEM(packet, f32),
            pltpu.VMEM(packet, f32),
            pltpu.VMEM(block, f32),
            pltpu.VMEM(block, f32),
            pltpu.VMEM(block, f32),
            pltpu.VMEM(block, f32),
            pltpu.VMEM(block, f32),
            pltpu.VMEM((seqs, features), bf16),
            pltpu.VMEM((seqs, w_gate.shape[1]), bf16),
            pltpu.SemaphoreType.DMA((9,)),
            pltpu.SemaphoreType.DMA((4,)),
            pltpu.SemaphoreType.DMA((4,)),
            pltpu.SemaphoreType.DMA((4,)),
            pltpu.SemaphoreType.DMA((4, n)),
            pltpu.SemaphoreType.DMA((4, n)),
        ],
        compiler_params=pltpu.CompilerParams(
            collective_id=0, has_side_effects=True, vmem_limit_bytes=60 * 1024 * 1024
        ),
    )(cache_lengths, expert_ids, *operands)


def solution(mesh):
    placed = (
        P("groups", None),
        P("groups", None),
        P("groups", None),
        P("groups", "seq", None),
        P("groups", "seq", None),
        P("groups"),
        P("groups", None),
        P("seq", None),
        P(),
        P(),
        P(None, "seq"),
        P(None, "seq"),
        P("seq", None),
        P("groups", None),
    )
    return jax.shard_map(
        functools.partial(fused_device, mesh.shape["seq"]),
        mesh=mesh,
        in_specs=placed,
        out_specs=(P("groups", "seq"), P("groups", "seq")),
        check_vma=False,
    )
```

```python
import functools
import math

import jax
import jax.numpy as jnp
from jax import lax
from jax.experimental import pallas as pl
from jax.experimental.pallas import tpu as pltpu
from jax.sharding import PartitionSpec as P

HEADS = 32
KV_HEADS = 8
HEAD_DIM = 128
FF = 7168


masked_score = -1e30


def joined(value, axis, join):
    pieces = jax.tree.map(lambda part: lax.all_gather(part, axis), value)
    head = jax.tree.map(lambda part: part[0], pieces)
    tail = jax.tree.map(lambda part: part[1:], pieces)
    so_far, _ = lax.scan(lambda so_far, share: (join(so_far, share), None), head, tail)
    return so_far


def merge_partial_results(first, second):
    first_max, first_sum, first_num = first
    second_max, second_sum, second_num = second
    ceiling = jnp.maximum(first_max, second_max)
    first_scale = jnp.exp(first_max - ceiling)
    second_scale = jnp.exp(second_max - ceiling)
    merged_sum = first_sum * first_scale + second_sum * second_scale
    merged_num = first_num * first_scale[..., None] + second_num * second_scale[..., None]
    return (ceiling, merged_sum, merged_num)


def per_device(
    query,
    new_key,
    new_value,
    cache_keys,
    cache_values,
    cache_lengths,
    residual_input,
    w_out,
    norm_gain,
    w_router,
    w_gate,
    w_up,
    expert_down_weight,
    expert_ids,
):
    seq_count = query.shape[0]
    per_group = HEADS // KV_HEADS
    local_len = cache_keys.shape[1]
    device = lax.axis_index("seq")
    inv_scale = 1.0 / math.sqrt(HEAD_DIM)
    query_vectors = query.reshape(seq_count, KV_HEADS, per_group, HEAD_DIM)
    key_block = cache_keys.reshape(seq_count, local_len, KV_HEADS, HEAD_DIM)
    value_block = cache_values.reshape(seq_count, local_len, KV_HEADS, HEAD_DIM)
    scores = (
        jnp.einsum("bkgd,btkd->bkgt", query_vectors, key_block, preferred_element_type=jnp.float32)
        * inv_scale
    )
    positions = device * local_len + jnp.arange(local_len, dtype=jnp.int32)
    is_live = (positions[None, :] < cache_lengths[:, None])[:, None, None, :]
    scores = jnp.where(is_live, scores, masked_score)
    incoming_key_rows = new_key.reshape(seq_count, KV_HEADS, HEAD_DIM)
    incoming_token_score = (
        jnp.einsum(
            "oqes,oqs->oqe", query_vectors, incoming_key_rows, preferred_element_type=jnp.float32
        )
        * inv_scale
    )
    fresh_value = new_value.astype(jnp.float32).reshape(seq_count, KV_HEADS, 1, HEAD_DIM)
    feat_width = w_out.shape[0]
    feat_start = device * feat_width
    flat_shape = (seq_count, HEADS * HEAD_DIM)
    local_max = jnp.max(scores, axis=-1)
    weights = jnp.where(is_live, jnp.exp(scores - local_max[..., None]), 0.0)
    numerator = jnp.einsum(
        "bkgt,btkd->bkgd",
        weights.astype(jnp.bfloat16),
        value_block,
        preferred_element_type=jnp.float32,
    )
    merged_max, merged_sum, merged_num = joined(
        (local_max, jnp.sum(weights, axis=-1), numerator), "seq", merge_partial_results
    )
    ceiling = jnp.maximum(merged_max, incoming_token_score)
    old_scale = jnp.exp(merged_max - ceiling)
    fresh_weight = jnp.exp(incoming_token_score - ceiling)
    fresh_rounded = lax.optimization_barrier(fresh_weight.astype(jnp.bfloat16)).astype(jnp.float32)
    numerator = merged_num * old_scale[..., None] + fresh_rounded[..., None] * fresh_value
    denominator = merged_sum * old_scale + fresh_weight
    context = (numerator / denominator[..., None]).reshape(flat_shape)
    context_own = lax.dynamic_slice_in_dim(context, feat_start, feat_width, 1).astype(jnp.bfloat16)
    projected = lax.psum(jnp.dot(context_own, w_out, preferred_element_type=jnp.float32), "seq")
    out_width = projected.shape[1] // lax.axis_size("seq")
    out_start = device * out_width
    attn_proj = lax.dynamic_slice_in_dim(projected, out_start, out_width, 1).astype(jnp.bfloat16)
    stream = residual_input.astype(jnp.float32) + projected
    normed = (
        stream
        * lax.rsqrt(jnp.mean(stream * stream, axis=-1, keepdims=True) + 1e-05)
        * norm_gain.astype(jnp.float32)
    )
    normed = normed.astype(jnp.bfloat16)
    logits = jnp.dot(normed, w_router, preferred_element_type=jnp.float32)
    expert_count = w_router.shape[1]
    picks = expert_ids[:, :, None] == jnp.arange(expert_count, dtype=jnp.int32)[None, None, :]
    chosen = jnp.sum(jnp.where(picks, logits[:, None, :], 0.0), axis=-1)
    first_gate = jax.nn.sigmoid(chosen[:, 0] - chosen[:, 1])
    gate_pair = jnp.stack([first_gate, 1.0 - first_gate], axis=1)
    own_expert = device * w_gate.shape[1] // FF
    route_weight = jnp.sum(jnp.where(expert_ids == own_expert, gate_pair, 0.0), axis=1)
    gate_part = jnp.dot(normed, w_gate, preferred_element_type=jnp.float32)
    up_projection_share = jnp.dot(normed, w_up, preferred_element_type=jnp.float32)
    hidden = (jax.nn.silu(gate_part) * up_projection_share).astype(jnp.bfloat16)
    term = lax.dot_general(
        expert_down_weight, hidden, (((0,), (1,)), ((), ())), preferred_element_type=jnp.float32
    )
    moe_rows = lax.psum_scatter(
        term * route_weight[None, :], "seq", scatter_dimension=0, tiled=True
    )
    stream_own = lax.dynamic_slice_in_dim(stream, out_start, out_width, 1)
    layer_out = (stream_own + moe_rows.T).astype(jnp.bfloat16)
    return (attn_proj, layer_out)


GROUP = 4


def xor_index(first, second, limit):
    result, bit = 0, 1
    while bit < limit:
        result = result + (first // bit + second // bit) % 2 * bit
        bit *= 2
    return result


def layer_kernel(
    n,
    lengths_ref,
    ids_ref,
    query_hbm,
    new_key_hbm,
    new_value_hbm,
    keys_hbm,
    values_hbm,
    residual_hbm,
    w_out_hbm,
    gain_hbm,
    router_hbm,
    gate_hbm,
    up_hbm,
    down_hbm,
    attn_out,
    layer_out,
    query,
    new_key,
    new_value,
    keys,
    values,
    residual,
    w_out,
    gain,
    router,
    w_gate,
    w_up,
    w_down,
    send_ctx,
    recv_ctx,
    send_proj,
    recv_proj,
    gathered,
    send_moe,
    recv_moe,
    scaled_ref,
    acc_gate,
    acc_up,
    hidden_ref,
    small_sem,
    gate_sem,
    up_sem,
    down_sem,
    send_sem,
    recv_sem,
):
    f32, bf16 = jnp.float32, jnp.bfloat16
    me = lax.axis_index("seq")
    seqs = query.shape[0]
    local_len = keys.shape[1]
    per_group = HEADS // KV_HEADS
    width = w_out.shape[0]
    own_heads = width // HEAD_DIM
    ff_local = w_gate.shape[1]
    inv_scale = 1.0 / math.sqrt(HEAD_DIM)

    small = [
        pltpu.make_async_copy(src, dst, small_sem.at[i])
        for i, (src, dst) in enumerate(
            (
                (query_hbm, query),
                (keys_hbm, keys),
                (values_hbm, values),
                (new_key_hbm, new_key),
                (new_value_hbm, new_value),
                (w_out_hbm, w_out),
                (residual_hbm, residual),
                (gain_hbm, gain),
                (router_hbm, router),
            )
        )
    ]
    for copy in small:
        copy.start()
    big = []
    for src, dst, sems in (
        (gate_hbm, w_gate, gate_sem),
        (up_hbm, w_up, up_sem),
        (down_hbm, w_down, down_sem),
    ):
        parts = sems.shape[0]
        rows = src.shape[0] // parts
        copies = [
            pltpu.make_async_copy(
                src.at[pl.ds(i * rows, rows)], dst.at[pl.ds(i * rows, rows)], sems.at[i]
            )
            for i in range(parts)
        ]
        for copy in copies:
            copy.start()
        big.append(copies)

    barrier = pltpu.get_barrier_semaphore()

    def greet(i, carry):
        pl.semaphore_signal(barrier, inc=1, device_id={"seq": lax.rem(me + i, n)})
        return carry

    lax.fori_loop(1, n, greet, 0)

    def exchange(phase, src, dst, peer, slot):
        return pltpu.make_async_remote_copy(
            src_ref=src,
            dst_ref=dst.at[slot],
            send_sem=send_sem.at[phase, peer],
            recv_sem=recv_sem.at[phase, slot],
            device_id={"seq": peer},
        )

    def wait_all(phase, dst):
        def step(i, carry):
            peer = xor_index(me, i, n)
            exchange(phase, dst.at[peer], dst, peer, peer).wait_recv()
            return carry

        lax.fori_loop(1, n, step, 0)

    rows = per_group * seqs
    cols = seqs * local_len
    row_seq = lax.rem(lax.broadcasted_iota(jnp.int32, (rows, 1), 0), seqs)
    row_len = jnp.zeros((rows, 1), jnp.int32)
    for b in range(seqs):
        row_len = jnp.where(row_seq == b, lengths_ref[b], row_len)
    offset = lax.broadcasted_iota(jnp.int32, (rows, cols), 1) - row_seq * local_len
    valid = (offset >= 0) & (offset < jnp.minimum(row_len - me * local_len, local_len))
    lane = lax.broadcasted_iota(jnp.int32, (rows, HEAD_DIM), 1)

    for copy in small[:3]:
        copy.wait()
    stats = [None] * HEADS
    for k in range(KV_HEADS):
        span = slice(k * HEAD_DIM, (k + 1) * HEAD_DIM)
        grouped = jnp.concatenate(
            [
                query[:, (k * per_group + g) * HEAD_DIM : (k * per_group + g + 1) * HEAD_DIM].astype(f32)
                for g in range(per_group)
            ],
            axis=0,
        ).astype(bf16)
        key_block = keys[:, :, span].reshape(cols, HEAD_DIM)
        value_block = values[:, :, span].reshape(cols, HEAD_DIM)
        scores = (
            lax.dot_general(
                grouped, key_block, (((1,), (1,)), ((), ())), preferred_element_type=f32
            )
            * inv_scale
        )
        scores = jnp.where(valid, scores, masked_score)
        top = jnp.max(scores, axis=1, keepdims=True)
        weights = jnp.where(valid, jnp.exp(scores - top), 0.0)
        total = jnp.sum(weights, axis=1, keepdims=True)
        numerator = jnp.dot(weights.astype(bf16), value_block, preferred_element_type=f32)
        for g in range(per_group):
            head = k * per_group + g
            peer, part = head // own_heads, head % own_heads
            part_rows = slice(g * seqs, (g + 1) * seqs)
            send_ctx[peer, :, part * HEAD_DIM : (part + 1) * HEAD_DIM] = numerator[part_rows]
            stats[head] = jnp.where(
                lane[:seqs] == 2 * part,
                top[part_rows],
                jnp.where(lane[:seqs] == 2 * part + 1, total[part_rows], 0.0),
            )
    for peer in range(n):
        block = stats[peer * own_heads]
        for part in range(1, own_heads):
            block = block + stats[peer * own_heads + part]
        send_ctx[peer, :, width:] = block

    pl.semaphore_wait(barrier, n - 1)

    def send_context(i, carry):
        peer = xor_index(me, n - i, n)
        exchange(0, send_ctx.at[peer], recv_ctx, peer, me).start()
        return carry

    lax.fori_loop(1, n, send_context, 0)
    recv_ctx[pl.ds(me, 1)] = send_ctx[pl.ds(me, 1)]

    for copy in small[3:5]:
        copy.wait()
    fresh = []
    for part in range(own_heads):
        head = me * own_heads + part
        kv = head // per_group
        at = pl.ds(pl.multiple_of(kv * HEAD_DIM, HEAD_DIM), HEAD_DIM)
        q_at = pl.ds(pl.multiple_of(head * HEAD_DIM, HEAD_DIM), HEAD_DIM)
        score = (
            jnp.sum(query[:, q_at].astype(f32) * new_key[:, at].astype(f32), axis=1, keepdims=True)
            * inv_scale
        )
        fresh.append((score, new_value[:, at].astype(f32)))

    wait_all(0, recv_ctx)
    pieces = []
    for part in range(own_heads):
        score, value = fresh[part]
        tops = recv_ctx[:, :, width + 2 * part : width + 2 * part + 1]
        totals = recv_ctx[:, :, width + 2 * part + 1 : width + 2 * part + 2]
        ceiling = jnp.maximum(jnp.max(tops, axis=0), score)
        scale = jnp.exp(tops - ceiling[None])
        new_weight = jnp.exp(score - ceiling)
        denominator = jnp.sum(totals * scale, axis=0) + new_weight
        numerator = jnp.sum(
            recv_ctx[:, :, part * HEAD_DIM : (part + 1) * HEAD_DIM] * scale, axis=0
        )
        numerator = numerator + new_weight.astype(bf16).astype(f32) * value
        pieces.append(numerator / denominator)
    context = jnp.concatenate(pieces, axis=1).astype(bf16)

    small[5].wait()

    products = jnp.dot(context, w_out[...], preferred_element_type=f32)
    for p in range(n):
        send_proj[p] = products[:, p * width : (p + 1) * width]

    def send_projected(i, carry):
        peer = xor_index(me, n - i, n)
        exchange(1, send_proj.at[peer], recv_proj, peer, me).start()
        return carry

    lax.fori_loop(1, n, send_projected, 0)
    recv_proj[pl.ds(me, 1)] = send_proj[pl.ds(me, 1)]
    for copy in small[6:]:
        copy.wait()
    wait_all(1, recv_proj)
    projected = jnp.sum(recv_proj[...], axis=0)
    gathered[me] = projected

    def send_gathered(i, carry):
        peer = xor_index(me, n - i, n)
        exchange(2, gathered.at[me], gathered, peer, me).start()
        return carry

    lax.fori_loop(1, n, send_gathered, 0)
    attn_out[...] = projected.astype(bf16)
    own_at = pl.ds(pl.multiple_of(me * width, width), width)
    stream_own = residual[:, own_at].astype(f32) + projected
    for copies in big[:2]:
        for copy in copies:
            copy.wait()

    groups = n // GROUP
    span = GROUP * width
    own_group = me // GROUP
    logit_shape = (seqs, router.shape[0])

    def absorb(i, carry):
        squares, logits = carry
        group = xor_index(own_group, i, groups)
        for q in range(GROUP):
            peer = group * GROUP + q

            @pl.when(peer != me)
            def _():
                exchange(2, gathered.at[peer], gathered, peer, peer).wait_recv()

        for q in range(GROUP):
            peer = group * GROUP + q
            at = pl.ds(pl.multiple_of(peer * width, width), width)
            stream = gathered[peer] + residual[:, at].astype(f32)
            squares = squares + stream * stream
            scaled_ref[group, :, q * width : (q + 1) * width] = (
                stream * gain[at].astype(f32).reshape(1, width)
            ).astype(bf16)
        scaled = scaled_ref[group]
        at = pl.ds(pl.multiple_of(group * span, span), span)
        logits = logits + lax.dot_general(
            scaled, router[:, at], (((1,), (1,)), ((), ())), preferred_element_type=f32
        )
        acc_gate[...] += jnp.dot(scaled, w_gate[at, :], preferred_element_type=f32)
        acc_up[...] += jnp.dot(scaled, w_up[at, :], preferred_element_type=f32)
        return squares, logits

    acc_gate[...] = jnp.zeros_like(acc_gate)
    acc_up[...] = jnp.zeros_like(acc_up)
    squares, logits = lax.fori_loop(
        0, groups, absorb, (jnp.zeros((seqs, width), f32), jnp.zeros(logit_shape, f32))
    )
    inv_rms = lax.rsqrt(jnp.sum(squares, axis=1, keepdims=True) / (n * width) + 1e-05)
    gate_part = acc_gate[...] * inv_rms
    hidden_ref[...] = (gate_part / (1.0 + jnp.exp(-gate_part)) * (acc_up[...] * inv_rms)).astype(bf16)

    logits = logits * inv_rms
    expert = lax.broadcasted_iota(jnp.int32, logits.shape, 1)
    token = lax.broadcasted_iota(jnp.int32, (seqs, 1), 0)
    first_id = jnp.zeros((seqs, 1), jnp.int32)
    second_id = jnp.zeros((seqs, 1), jnp.int32)
    for b in range(seqs):
        first_id = jnp.where(token == b, ids_ref[0, b], first_id)
        second_id = jnp.where(token == b, ids_ref[1, b], second_id)
    first_logit = jnp.sum(jnp.where(expert == first_id, logits, 0.0), axis=1, keepdims=True)
    second_logit = jnp.sum(jnp.where(expert == second_id, logits, 0.0), axis=1, keepdims=True)
    first_gate = 1.0 / (1.0 + jnp.exp(second_logit - first_logit))
    own_expert = me * ff_local // FF
    route = jnp.where(first_id == own_expert, first_gate, 0.0) + jnp.where(
        second_id == own_expert, 1.0 - first_gate, 0.0
    )
    for copy in big[2]:
        copy.wait()

    def send_contributions(i, carry):
        group = xor_index(own_group, groups - 1 - i, groups)
        at = pl.ds(pl.multiple_of(group * span, span), span)
        terms = jnp.dot(hidden_ref[...], w_down[:, at], preferred_element_type=f32) * route
        for q in range(GROUP):
            peer = group * GROUP + q
            send_moe[peer] = terms[:, q * width : (q + 1) * width]

            @pl.when(peer != me)
            def _():
                exchange(3, send_moe.at[peer], recv_moe, peer, me).start()

        return carry

    lax.fori_loop(0, groups, send_contributions, 0)
    recv_moe[pl.ds(me, 1)] = send_moe[pl.ds(me, 1)]
    wait_all(3, recv_moe)
    layer_out[...] = (stream_own + jnp.sum(recv_moe[...], axis=0)).astype(bf16)

    def finish(i, carry):
        peer = lax.rem(me + i, n)
        exchange(0, send_ctx.at[peer], recv_ctx, peer, me).wait_send()
        exchange(1, send_proj.at[peer], recv_proj, peer, me).wait_send()
        exchange(2, gathered.at[me], gathered, peer, me).wait_send()
        exchange(3, send_moe.at[peer], recv_moe, peer, me).wait_send()
        return carry

    lax.fori_loop(1, n, finish, 0)


def emit_kernel(attn_ref, layer_ref, attn_out, layer_out):
    attn_out[...] = attn_ref[...]
    layer_out[...] = layer_ref[...]


def fused_device(n, *args):
    (
        query,
        new_key,
        new_value,
        cache_keys,
        cache_values,
        cache_lengths,
        residual_input,
        w_out,
        norm_gain,
        w_router,
        w_gate,
        w_up,
        expert_down_weight,
        expert_ids,
    ) = args
    seqs, features = residual_input.shape
    width = w_out.shape[0]
    if n < 2 * GROUP or n & (n - 1) or width % HEAD_DIM or FF % w_gate.shape[1] or width * n != features or cache_keys.shape[1] % 16:
        return per_device(*args)
    f32, bf16 = jnp.float32, jnp.bfloat16
    operands = (
        query,
        new_key,
        new_value,
        cache_keys,
        cache_values,
        residual_input,
        w_out,
        norm_gain,
        w_router.T,
        w_gate,
        w_up,
        expert_down_weight,
    )
    packet = (n, seqs, width + HEAD_DIM)
    block = (n, seqs, width)
    out = jax.ShapeDtypeStruct((seqs, width), bf16)
    results = pl.pallas_call(
        functools.partial(layer_kernel, n),
        out_shape=(out, out),
        in_specs=[pl.BlockSpec(memory_space=pltpu.SMEM)] * 2
        + [pl.BlockSpec(memory_space=pl.ANY)] * len(operands),
        out_specs=(pl.BlockSpec(memory_space=pltpu.VMEM),) * 2,
        scratch_shapes=[pltpu.VMEM(x.shape, x.dtype) for x in operands]
        + [
            pltpu.VMEM(packet, f32),
            pltpu.VMEM(packet, f32),
            pltpu.VMEM(block, f32),
            pltpu.VMEM(block, f32),
            pltpu.VMEM(block, f32),
            pltpu.VMEM(block, f32),
            pltpu.VMEM(block, f32),
            pltpu.VMEM((n // GROUP, seqs, GROUP * width), bf16),
            pltpu.VMEM((seqs, w_gate.shape[1]), f32),
            pltpu.VMEM((seqs, w_gate.shape[1]), f32),
            pltpu.VMEM((seqs, w_gate.shape[1]), bf16),
            pltpu.SemaphoreType.DMA((9,)),
            pltpu.SemaphoreType.DMA((4,)),
            pltpu.SemaphoreType.DMA((4,)),
            pltpu.SemaphoreType.DMA((4,)),
            pltpu.SemaphoreType.DMA((4, n)),
            pltpu.SemaphoreType.DMA((4, n)),
        ],
        compiler_params=pltpu.CompilerParams(
            collective_id=0, has_side_effects=True, vmem_limit_bytes=60 * 1024 * 1024
        ),
    )(cache_lengths, expert_ids.T, *operands)
    return pl.pallas_call(
        emit_kernel,
        out_shape=(out, out),
        in_specs=[pl.BlockSpec(memory_space=pltpu.VMEM)] * 2,
        out_specs=(pl.BlockSpec(memory_space=pltpu.VMEM),) * 2,
    )(*results)


def solution(mesh):
    placed = (
        P("groups", None),
        P("groups", None),
        P("groups", None),
        P("groups", "seq", None),
        P("groups", "seq", None),
        P("groups"),
        P("groups", None),
        P("seq", None),
        P(),
        P(),
        P(None, "seq"),
        P(None, "seq"),
        P("seq", None),
        P("groups", None),
    )
    return jax.shard_map(
        functools.partial(fused_device, mesh.shape["seq"]),
        mesh=mesh,
        in_specs=placed,
        out_specs=(P("groups", "seq"), P("groups", "seq")),
        check_vma=False,
    )
```
